32 devices in a mesh: expert: 16 (over z, x, core), dp: 2 (over y).
Axes of the slice: x: 2, y: 2, z: 4, core: 2. Of those that a mesh axis runs over, the one named last changes fastest.
Arguments:
- tokens: bfloat16 [4096, 2560], P(('expert', 'dp')), may hold values from -6 to 6
- routes: int32 [4096, 2], P(('expert', 'dp')), may hold values from 0 to 3, all different within a row; in each aligned block of 128 rows (0 to 127, 128 to 255, ...) at most 88 rows name the same one
- combine_weight: float32 [4096, 2], P(('expert', 'dp')), may hold values from 0.05 to 1
- owner_plan: int32 [4], replicated, may hold values from 0 to 3, as said below
- w_in: bfloat16 [2, 3072, 2560], P(None, 'expert', 'dp'), may hold values from -0.125 to 0.125
- w_out: bfloat16 [3072, 2560], P('expert', 'dp'), may hold values from -0.21875 to 0.21875
- grad_in: bfloat16 [2, 2, 3072, 2560], P('dp', None, 'expert'), may hold values from -6 to 6
- grad_out: bfloat16 [2, 3072, 2560], P('dp', 'expert'), may hold values from -6 to 6
- first_in: bfloat16 [2, 3072, 2560], P(None, 'expert', 'dp'), may hold values from -3 to 3
- second_in: bfloat16 [2, 3072, 2560], P(None, 'expert', 'dp'), may hold values from 0.25 to 4
- first_out: bfloat16 [3072, 2560], P('expert', 'dp'), may hold values from -3 to 3
- second_out: bfloat16 [3072, 2560], P('expert', 'dp'), may hold values from 0.25 to 4
Outputs:
- combined: bfloat16 [4096, 2560], P(('expert', 'dp'))
- first_in_next: bfloat16 [2, 3072, 2560], P(None, 'expert', 'dp')
- second_in_next: bfloat16 [2, 3072, 2560], P(None, 'expert', 'dp')
- first_out_next: bfloat16 [3072, 2560], P('expert', 'dp')
- second_out_next: bfloat16 [3072, 2560], P('expert', 'dp')
The draws below stay inside these ranges and needn't reach their ends.
Inputs may be any that keep to these rules, and one draw needn't show every extreme that they name: owner_plan is an involution: exactly 2 pairs of experts trade owners, every other expert maps to itself. `routes`: in the rows of one device (128 rows) no expert is named by more than 88 rows, a bound that some expert reaches in some device.
All inputs are finite; a program needn't handle non-finite values.
Results may differ from the reference program's by a relative error of at most 0.014.
Values may be sent and summed in bfloat16 or wider, within the bound.
A program may use at most 192 MiB of HBM per device.

```python
import math
import jax
import jax.numpy as jnp
import numpy as np
from jax import lax

D = 2560
HID = 768
GROUP = 4
TOK_DEV = 128
HDEV = 192
EXPERTS = 4
TOP = 2
MOVED = 2
CAP = 88
TOKENS = 4096
N_DP = 2
DEVICES = 32


def draw_owner_plan(key, part):
    shuffled = jax.random.permutation(jax.random.fold_in(key, 7), EXPERTS).astype(jnp.int32)
    expert_ids = jnp.arange(EXPERTS, dtype=jnp.int32)
    leaving = shuffled[:MOVED]
    arriving = shuffled[MOVED:2 * MOVED]
    owner_plan = expert_ids.at[leaving].set(arriving).at[arriving].set(leaving)
    return owner_plan.astype(jnp.int32)


def shard_levels(stream_key, dims, cuts, low, top_value):
    factor_of = 1.0
    for axis_at, parts in cuts:
        heights = jax.random.uniform(jax.random.fold_in(jax.random.fold_in(stream_key, 6), axis_at), (parts,), jnp.float32, low / len(cuts), top_value / len(cuts))
        factor_of = factor_of * jnp.repeat(jnp.exp(heights), dims[axis_at] // parts).reshape((-1,) + (1,) * (len(dims) - 1 - axis_at))
    return factor_of


def deal_out(key, own, number, rows, number_of, top, bound, slope):
    order = jax.random.permutation(key, number_of)
    packed, common = portions_of(number_of, rows * top, bound, slope, True), portions_of(number_of, rows * top, bound, slope, False)
    places = jnp.arange(number_of)

    def named(lengths, offset_by):
        used = int((lengths > 0).sum())
        fixed = max(1, used // 4)
        moved = fixed + (places - fixed + offset_by * (used - fixed)) % max(1, number_of - fixed)
        return jnp.zeros((number_of,), jnp.int32).at[order[jnp.where(places < fixed, places, moved)]].set(jnp.asarray(lengths, jnp.int32))

    lengths = jnp.where(number % 4 == 0, named(packed, number // 4), named(common, number - number // 4 - 1))
    mixed = jax.random.permutation(jax.random.fold_in(own, 3), number_of)
    giver, taker = mixed[0:number_of // 2 * 2:2], mixed[1:number_of // 2 * 2:2]
    slack = jnp.minimum(lengths[giver] - 1, bound - lengths[taker]) // 2
    slack = jnp.where((giver == order[0]) | (taker == order[0]) | (lengths[taker] == 0), 0, jnp.maximum(slack, 0))
    moved = jax.random.randint(jax.random.fold_in(own, 4), (number_of // 2,), 0, 1 << 20) % (slack + 1)
    lengths = lengths.at[giver].add(-moved).at[taker].add(moved)
    members = jnp.searchsorted(jnp.cumsum(lengths), jnp.arange(rows * top), side="right").astype(jnp.int32)
    listing = members.reshape(top, rows).T
    listing = listing[jax.random.permutation(jax.random.fold_in(own, 1), rows)]
    offset_by = jax.random.randint(jax.random.fold_in(own, 2), (rows, 1), 0, top)
    return jnp.take_along_axis(listing, (jnp.arange(top)[None, :] + offset_by) % top, axis=1)


def portions_of(amount, total, bound, slope, full):
    loads = [(1 << 20) // math.isqrt(rank ** slope) + 1 for rank in range(1, amount + 1)]
    largest = bound if full else min(bound, max(-(-total // amount), total * loads[0] // sum(loads)))
    least = 1 if total - largest >= amount - 1 else 0
    counts, rest = [largest] + [least] * (amount - 1), total - largest - least * (amount - 1)
    while rest > 0:
        candidates = [i for i in range(1, amount) if counts[i] < largest] or [i for i in range(1, amount) if counts[i] < bound]
        pool, left = sum([loads[i] for i in candidates]), rest
        for i in candidates:
            extra = min(bound - counts[i], max(1, left * loads[i] // pool), rest)
            counts[i] = counts[i] + extra
            rest = rest - extra
    return np.array(counts)


def noise(rng, extent, scale, limit, shards=(), held_as=jnp.bfloat16):
    array = jax.random.normal(rng, extent, jnp.float32) * scale
    if len(shards) > 0:
        array = shard_levels(rng, extent, shards, -0.22, 0.18) * array
    return jnp.clip(array, min=-limit, max=limit).astype(held_as)


def setup_inputs(seed: int = 0) -> dict:
    keys = jax.random.split(jax.random.key(seed), 13)
    tokens = noise(keys[0], (TOKENS, D), 1.0, 6.0, ((0, 32),))
    routes_keys = jax.random.split(jax.random.fold_in(keys[1], 1), TOKENS // TOK_DEV)
    routes_turns = jax.random.permutation(jax.random.fold_in(keys[1], 3), TOKENS // TOK_DEV)
    routes = jax.vmap(lambda own, number: deal_out(jax.random.fold_in(keys[1], 2), own, number, TOK_DEV, EXPERTS, TOP, CAP, 2))(routes_keys, routes_turns).reshape((TOKENS, TOP))
    combine_weight = jnp.clip(jnp.exp(math.log(1.0) - 2.9957323 * jax.random.uniform(keys[2], (TOKENS, TOP), jnp.float32) ** shard_levels(keys[2], (TOKENS, TOP), ((0, 32),), -0.2, 0.2)), 0.05, 1.0)
    owner_plan = draw_owner_plan(jax.random.fold_in(keys[12], 71), 0)
    w_in = noise(keys[4], (2, EXPERTS * HID, D), D ** -0.5, 0.125, ((1, 16), (2, 2)))
    w_out = noise(keys[5], (EXPERTS * HID, D), HID ** -0.5, 0.21875, ((0, 16), (1, 2)))
    grad_in = noise(keys[6], (N_DP, 2, EXPERTS * HID, D), 1.0, 6.0, ((0, 2), (2, 16)))
    grad_out = noise(keys[7], (N_DP, EXPERTS * HID, D), 1.0, 6.0, ((0, 2), (1, 16)))
    first_in = noise(keys[8], (2, EXPERTS * HID, D), 0.5, 3.0, ((1, 16), (2, 2)))
    second_in = jnp.clip(jnp.exp(math.log(4.0) - 2.7725887 * jax.random.uniform(keys[9], (2, EXPERTS * HID, D), jnp.float32) ** shard_levels(keys[9], (2, EXPERTS * HID, D), ((1, 16), (2, 2)), -0.2, 0.2)), 0.25, 4.0).astype(jnp.bfloat16)
    first_out = noise(keys[10], (EXPERTS * HID, D), 0.5, 3.0, ((0, 16), (1, 2)))
    second_out = jnp.clip(jnp.exp(math.log(4.0) - 2.7725887 * jax.random.uniform(keys[11], (EXPERTS * HID, D), jnp.float32) ** shard_levels(keys[11], (EXPERTS * HID, D), ((0, 16), (1, 2)), -0.2, 0.2)), 0.25, 4.0).astype(jnp.bfloat16)
    return dict(tokens=tokens, routes=routes, combine_weight=combine_weight, owner_plan=owner_plan, w_in=w_in, w_out=w_out, grad_in=grad_in, grad_out=grad_out, first_in=first_in, second_in=second_in, first_out=first_out, second_out=second_out)


BETA_ONE = 0.9
BETA_TWO = 0.95
LEARNING_RATE = 0.005
EPSILON = 1e-08
CORRECT_FIRST = 1.0 / (1.0 - 0.9 ** 10)
CORRECT_SECOND = 1.0 / (1.0 - 0.95 ** 10)

def adam_update(weight, gradient, first_moment, second_moment):
    first_next = BETA_ONE * first_moment.astype(jnp.float32) + (1.0 - BETA_ONE) * gradient
    second_next = BETA_TWO * second_moment.astype(jnp.float32) + (1.0 - BETA_TWO) * gradient * gradient
    stepped = weight.astype(jnp.float32) - LEARNING_RATE * (first_next * CORRECT_FIRST) / (jnp.sqrt(second_next * CORRECT_SECOND) + EPSILON)
    return (stepped.astype(jnp.bfloat16), first_next.astype(jnp.bfloat16), second_next.astype(jnp.bfloat16))

def slot_ranks(flat_routes):
    onehot = (flat_routes[:, None] == jnp.arange(EXPERTS, dtype=jnp.int32)[None, :]).astype(jnp.int32)
    ranks = jnp.cumsum(onehot, axis=0) - 1
    return lax.optimization_barrier(jnp.sum(ranks * onehot, axis=1)).astype(jnp.int32)

def times_rows(row_data, weight_rows):
    return lax.dot_general(row_data, weight_rows, (((1,), (1,)), ((), ())), preferred_element_type=jnp.float32)

def expert_rows(row_data, weight_in, weight_out):
    gate = times_rows(row_data, weight_in[0])
    upward = times_rows(row_data, weight_in[1])
    hidden = (jax.nn.silu(gate) * upward).astype(jnp.bfloat16)
    return jnp.dot(hidden, weight_out, preferred_element_type=jnp.float32).astype(jnp.bfloat16)

def expert_output(row_data, weight_in, weight_out):
    total = jnp.zeros((row_data.shape[0], weight_out.shape[1]), jnp.float32)
    for quarter in range(GROUP):
        begin = quarter * HDEV
        total = total + expert_rows(row_data, weight_in[:, begin:begin + HDEV], weight_out[begin:begin + HDEV]).astype(jnp.float32)
    return total.astype(jnp.bfloat16)

def reference(tokens, routes, combine_weight, owner_plan, w_in, w_out, grad_in, grad_out, first_in, second_in, first_out, second_out):
    width = tokens.shape[1]
    sum_in = lax.optimization_barrier(jnp.sum(grad_in.astype(jnp.float32), axis=0))
    sum_out = lax.optimization_barrier(jnp.sum(grad_out.astype(jnp.float32), axis=0))
    new_in, first_in_next, second_in_next = adam_update(w_in, sum_in, first_in, second_in)
    new_out, first_out_next, second_out_next = adam_update(w_out, sum_out, first_out, second_out)

    def regroup_in(moment):
        return jnp.take(moment.reshape(2, EXPERTS, HID, width), owner_plan, axis=1).reshape(moment.shape)

    def regroup_out(moment):
        return jnp.take(moment.reshape(EXPERTS, HID, width), owner_plan, axis=0).reshape(moment.shape)
    device_routes = routes.reshape(DEVICES, TOK_DEV * TOP)
    ranks = jax.vmap(slot_ranks)(device_routes)
    targets = (device_routes * CAP + ranks).astype(jnp.int32)
    token_ids = jnp.arange(TOKENS, dtype=jnp.int32).reshape(DEVICES, TOK_DEV)
    token_of_route = jnp.repeat(token_ids, TOP, axis=1)
    device_ids = jnp.repeat(jnp.arange(DEVICES, dtype=jnp.int32)[:, None], TOK_DEV * TOP, axis=1)
    table = jnp.zeros((DEVICES, EXPERTS * CAP), jnp.int32).at[device_ids, targets].set(token_of_route)
    weight_table = jnp.zeros((DEVICES, EXPERTS * CAP), jnp.float32).at[device_ids, targets].set(combine_weight.reshape(DEVICES, TOK_DEV * TOP))

    def one_expert(total, expert):
        start = (expert * CAP).astype(jnp.int32)
        row_ids = lax.dynamic_slice_in_dim(table, start, CAP, 1).reshape(-1)
        row_weights = lax.dynamic_slice_in_dim(weight_table, start, CAP, 1).reshape(-1)
        weight_in = lax.dynamic_slice_in_dim(new_in, (expert * HID).astype(jnp.int32), HID, 1)
        weight_out = lax.dynamic_slice_in_dim(new_out, (expert * HID).astype(jnp.int32), HID, 0)
        result = expert_output(tokens[row_ids], weight_in, weight_out)
        return (total.at[row_ids].add(row_weights[:, None] * result.astype(jnp.float32)), None)
    total, ignored = lax.scan(one_expert, jnp.zeros((TOKENS, width), jnp.float32), jnp.arange(EXPERTS, dtype=jnp.int32))
    return (total.astype(jnp.bfloat16), regroup_in(first_in_next), regroup_in(second_in_next), regroup_out(first_out_next), regroup_out(second_out_next))
```

```python
import jax
import jax.numpy as jnp
from jax import lax
from jax.sharding import PartitionSpec as P

GROUP = 4

BETA_ONE = 0.9
BETA_TWO = 0.95
LEARNING_RATE = 0.005
EPSILON = 1e-08
CORRECT_FIRST = 1.0 / (1.0 - 0.9**10)
CORRECT_SECOND = 1.0 / (1.0 - 0.95**10)


def exchanged(block, axis, mask):
    return lax.ppermute(block, axis, [(i, i ^ mask) for i in range(lax.axis_size(axis))])


def adam_update(weight, gradient, first_moment, second_moment):
    first_next = BETA_ONE * first_moment.astype(jnp.float32) + (1.0 - BETA_ONE) * gradient
    second_next = (
        BETA_TWO * second_moment.astype(jnp.float32) + (1.0 - BETA_TWO) * gradient * gradient
    )
    stepped = weight.astype(jnp.float32) - LEARNING_RATE * (first_next * CORRECT_FIRST) / (
        jnp.sqrt(second_next * CORRECT_SECOND) + EPSILON
    )
    return (
        stepped.astype(jnp.bfloat16),
        first_next.astype(jnp.bfloat16),
        second_next.astype(jnp.bfloat16),
    )


def slot_ranks(flat_routes, expert_count):
    onehot = (flat_routes[:, None] == jnp.arange(expert_count, dtype=jnp.int32)[None, :]).astype(
        jnp.int32
    )
    ranks = jnp.cumsum(onehot, axis=0) - 1
    return jnp.sum(ranks * onehot, axis=1)


def times_rows(row_data, weight_rows):
    return lax.dot_general(
        row_data, weight_rows, (((1,), (1,)), ((), ())), preferred_element_type=jnp.float32
    )


def migrate_any(moment, source_rows, device_count):
    spread = lax.all_to_all(
        moment.reshape(device_count, -1), "expert", split_axis=0, concat_axis=0, tiled=True
    )
    picked = jnp.take(spread, source_rows, axis=0)
    landed = lax.all_to_all(picked, "expert", split_axis=0, concat_axis=0, tiled=True)
    return landed.reshape(moment.shape)


def summed_half(gradient, dp_index):
    half = gradient.shape[1] // 2
    kept = lax.dynamic_slice_in_dim(gradient, dp_index * half, half, 1)
    leaving = lax.dynamic_slice_in_dim(gradient, (1 - dp_index) * half, half, 1)
    return kept.astype(jnp.float32) + exchanged(leaving, "dp", 1).astype(jnp.float32)


def gathered(piece):
    pieces = {(0, 0): piece, (0, 1): exchanged(piece, "dp", 1)}
    for side in range(2):
        pieces[2, side] = exchanged(pieces[0, side], "expert", 2)
    for side in range(2):
        pieces[1, side] = exchanged(pieces[0, side], "expert", 1)
        pieces[3, side] = exchanged(pieces[2, side], "expert", 1)
    return pieces


def body(
    move,
    tokens,
    routes,
    combine_weight,
    w_in,
    w_out,
    grad_in,
    grad_out,
    first_in,
    second_in,
    first_out,
    second_out,
):
    device_count = lax.axis_size("expert")
    expert_count = device_count // GROUP
    token_count, route_count = routes.shape
    width = tokens.shape[1]
    half = width // 2
    capacity = GROUP * (
        (token_count * route_count * 4 + 3 * expert_count * GROUP - 1) // (3 * expert_count * GROUP)
    )
    dp_index = lax.axis_index("dp")
    my_group = lax.axis_index("expert") // GROUP

    flat_routes = routes.reshape(-1)
    ranks = slot_ranks(flat_routes, expert_count)
    relative = flat_routes ^ my_group
    targets = (relative * capacity + ranks).reshape(token_count, route_count)
    slot_ids = jnp.arange(expert_count * capacity, dtype=jnp.int32)
    selector = jnp.any(targets[None, :, :] == slot_ids[:, None, None], axis=2).astype(jnp.bfloat16)
    outgoing = jnp.dot(selector, tokens, preferred_element_type=jnp.float32).astype(jnp.bfloat16)
    outgoing = outgoing.reshape(expert_count, capacity, width)
    arrived = [outgoing[0]] + [
        exchanged(outgoing[mask], "expert", mask * GROUP) for mask in range(1, expert_count)
    ]

    weights = (w_in[0], w_in[1], w_out)
    gradients = (grad_in[0, 0], grad_in[0, 1], grad_out[0])
    firsts = (first_in[0], first_in[1], first_out)
    seconds = (second_in[0], second_in[1], second_out)
    sums = [summed_half(gradient, dp_index) for gradient in gradients]
    stepped = [adam_update(*arrays) for arrays in zip(weights, sums, firsts, seconds)]
    gate_pieces, up_pieces, out_pieces = [gathered(step[0]) for step in stepped]
    moved_first = [move(step[1]) for step in stepped]
    moved_second = [move(step[2]) for step in stepped]

    rows = jnp.concatenate(arrived, 0)
    sides = [
        lax.dynamic_slice_in_dim(rows, dp_index * half, half, 1),
        lax.dynamic_slice_in_dim(rows, (1 - dp_index) * half, half, 1),
    ]
    totals = [jnp.zeros((rows.shape[0], half), jnp.float32) for _ in range(2)]
    for quarter in (0, 1, 2, 3):
        gate = times_rows(sides[0], gate_pieces[quarter, 0]) + times_rows(
            sides[1], gate_pieces[quarter, 1]
        )
        upward = times_rows(sides[0], up_pieces[quarter, 0]) + times_rows(
            sides[1], up_pieces[quarter, 1]
        )
        hidden = (jax.nn.silu(gate) * upward).astype(jnp.bfloat16)
        for side in range(2):
            part = jnp.dot(
                hidden, out_pieces[quarter, side], preferred_element_type=jnp.float32
            ).astype(jnp.bfloat16)
            totals[side] = totals[side] + part.astype(jnp.float32)
    near, far = [total.astype(jnp.bfloat16) for total in totals]
    results = jnp.where(
        dp_index == 0, jnp.concatenate([near, far], 1), jnp.concatenate([far, near], 1)
    ).reshape(expert_count, capacity, width)
    returned = [results[0]] + [
        exchanged(results[mask], "expert", mask * GROUP) for mask in range(1, expert_count)
    ]
    by_slot = jnp.concatenate(returned, 0)
    weight_table = jnp.sum(
        jnp.where(targets[:, :, None] == slot_ids[None, None, :], combine_weight[:, :, None], 0.0),
        axis=1,
    )
    weight_high = weight_table.astype(jnp.bfloat16)
    weight_low = (weight_table - weight_high.astype(jnp.float32)).astype(jnp.bfloat16)
    combined = (
        jnp.dot(weight_high, by_slot, preferred_element_type=jnp.float32)
        + jnp.dot(weight_low, by_slot, preferred_element_type=jnp.float32)
    ).astype(jnp.bfloat16)
    return (
        combined,
        jnp.stack(moved_first[:2]),
        jnp.stack(moved_second[:2]),
        moved_first[2],
        moved_second[2],
    )


def local(tokens, routes, combine_weight, owner_plan, *state):
    device_count = lax.axis_size("expert")
    expert_count = device_count // GROUP
    operands = (tokens, routes, combine_weight) + state
    if expert_count == 4:
        branches = [
            lambda *arrays, mask=mask: body(
                lambda moment: exchanged(moment, "expert", mask * GROUP), *arrays
            )
            for mask in range(1, expert_count)
        ]
        return lax.switch(owner_plan[0] - 1, branches, *operands)
    device_ids = jnp.arange(device_count, dtype=jnp.int32)
    source_rows = jnp.take(owner_plan, device_ids // GROUP) * GROUP + device_ids % GROUP
    return body(lambda moment: migrate_any(moment, source_rows, device_count), *operands)


def solution(mesh):
    in_specs = (
        P(("expert", "dp"), None),
        P(("expert", "dp"), None),
        P(("expert", "dp"), None),
        P(),
        P(None, "expert", "dp"),
        P("expert", "dp"),
        P("dp", None, "expert", None),
        P("dp", "expert", None),
        P(None, "expert", "dp"),
        P(None, "expert", "dp"),
        P("expert", "dp"),
        P("expert", "dp"),
    )
    out_specs = (
        P(("expert", "dp"), None),
        P(None, "expert", "dp"),
        P(None, "expert", "dp"),
        P("expert", "dp"),
        P("expert", "dp"),
    )
    return jax.shard_map(local, mesh=mesh, in_specs=in_specs, out_specs=out_specs, check_vma=False)
```

```python
import jax
import jax.numpy as jnp
from jax import lax
from jax.sharding import PartitionSpec as P

GROUP = 4

BETA_ONE = 0.9
BETA_TWO = 0.95
LEARNING_RATE = 0.005
EPSILON = 1e-08
CORRECT_FIRST = 1.0 / (1.0 - 0.9**10)
CORRECT_SECOND = 1.0 / (1.0 - 0.95**10)


def exchanged(block, axis, mask):
    return lax.ppermute(block, axis, [(i, i ^ mask) for i in range(lax.axis_size(axis))])


def adam_update(weight, gradient, first_moment, second_moment):
    first_next = BETA_ONE * first_moment.astype(jnp.float32) + (1.0 - BETA_ONE) * gradient
    second_next = (
        BETA_TWO * second_moment.astype(jnp.float32) + (1.0 - BETA_TWO) * gradient * gradient
    )
    stepped = weight.astype(jnp.float32) - LEARNING_RATE * (first_next * CORRECT_FIRST) / (
        jnp.sqrt(second_next * CORRECT_SECOND) + EPSILON
    )
    return (
        stepped.astype(jnp.bfloat16),
        first_next.astype(jnp.bfloat16),
        second_next.astype(jnp.bfloat16),
    )


def slot_ranks(flat_routes, expert_count):
    onehot = (flat_routes[:, None] == jnp.arange(expert_count, dtype=jnp.int32)[None, :]).astype(
        jnp.int32
    )
    ranks = jnp.cumsum(onehot, axis=0) - 1
    return jnp.sum(ranks * onehot, axis=1)


def times_rows(row_data, weight_rows):
    return lax.dot_general(
        row_data, weight_rows, (((1,), (1,)), ((), ())), preferred_element_type=jnp.float32
    )


def migrate_any(moment, source_rows, device_count):
    spread = lax.all_to_all(
        moment.reshape(device_count, -1), "expert", split_axis=0, concat_axis=0, tiled=True
    )
    picked = jnp.take(spread, source_rows, axis=0)
    landed = lax.all_to_all(picked, "expert", split_axis=0, concat_axis=0, tiled=True)
    return landed.reshape(moment.shape)


def halves(gradient, dp_index):
    half = gradient.shape[1] // 2
    kept = lax.dynamic_slice_in_dim(gradient, dp_index * half, half, 1)
    leaving = lax.dynamic_slice_in_dim(gradient, (1 - dp_index) * half, half, 1)
    return kept, leaving


def slot_targets(routes, my_group, expert_count, capacity):
    flat_routes = routes.reshape(-1)
    ranks = slot_ranks(flat_routes, expert_count)
    return ((flat_routes ^ my_group) * capacity + ranks).reshape(routes.shape)


def slot_rows(tokens, targets, slot_count):
    slot_ids = jnp.arange(slot_count, dtype=jnp.int32)
    selector = jnp.any(targets[None, :, :] == slot_ids[:, None, None], axis=2).astype(jnp.bfloat16)
    return jnp.dot(selector, tokens, preferred_element_type=jnp.float32).astype(jnp.bfloat16)


def weighted(targets, combine_weight, by_slot):
    slot_ids = jnp.arange(by_slot.shape[0], dtype=jnp.int32)
    weight_table = jnp.sum(
        jnp.where(targets[:, :, None] == slot_ids[None, None, :], combine_weight[:, :, None], 0.0),
        axis=1,
    )
    weight_high = weight_table.astype(jnp.bfloat16)
    weight_low = (weight_table - weight_high.astype(jnp.float32)).astype(jnp.bfloat16)
    return jnp.dot(weight_high, by_slot, preferred_element_type=jnp.float32) + jnp.dot(
        weight_low, by_slot, preferred_element_type=jnp.float32
    )


def gathered(piece):
    pieces = {(0, 0): piece, (0, 1): exchanged(piece, "dp", 1)}
    for side in range(2):
        pieces[2, side] = exchanged(pieces[0, side], "expert", 2)
    for side in range(2):
        pieces[1, side] = exchanged(pieces[0, side], "expert", 1)
        pieces[3, side] = exchanged(pieces[2, side], "expert", 1)
    return pieces


def body(
    move,
    relay,
    tokens,
    routes,
    combine_weight,
    w_in,
    w_out,
    grad_in,
    grad_out,
    first_in,
    second_in,
    first_out,
    second_out,
):
    device_count = lax.axis_size("expert")
    expert_count = device_count // GROUP
    token_count, route_count = routes.shape
    width = tokens.shape[1]
    half = width // 2
    capacity = GROUP * (
        (token_count * route_count * 4 + 3 * expert_count * GROUP - 1) // (3 * expert_count * GROUP)
    )
    dp_index = lax.axis_index("dp")
    my_group = lax.axis_index("expert") // GROUP

    gradients = (grad_out[0], grad_in[0, 0], grad_in[0, 1])
    split = [halves(gradient, dp_index) for gradient in gradients]
    *leaving, tokens, routes = lax.optimization_barrier(
        tuple(pair[1] for pair in split) + (tokens, routes)
    )
    received = [exchanged(block, "dp", 1) for block in leaving]

    targets = slot_targets(routes, my_group, expert_count, capacity)
    if relay:
        far_tokens = exchanged(tokens, "expert", 3 * GROUP)
        far_small = exchanged(
            jnp.concatenate([routes.astype(jnp.float32), combine_weight], 1), "expert", 3 * GROUP
        )
        far_routes = far_small[:, :route_count].astype(jnp.int32)
        far_weight = far_small[:, route_count:]
        far_targets = slot_targets(far_routes, my_group, expert_count, capacity)
        near = slot_rows(tokens, targets, 2 * capacity)
        far = slot_rows(far_tokens, far_targets, 2 * capacity)
        arrived = [
            near[:capacity],
            exchanged(near[capacity:], "expert", GROUP),
            far[:capacity],
            exchanged(far[capacity:], "expert", GROUP),
        ]
    else:
        outgoing = slot_rows(tokens, targets, expert_count * capacity)
        outgoing = outgoing.reshape(expert_count, capacity, width)
        arrived = [outgoing[0]] + [
            exchanged(outgoing[mask], "expert", mask * GROUP) for mask in range(1, expert_count)
        ]

    weights = (w_out, w_in[0], w_in[1])
    firsts = (first_out, first_in[0], first_in[1])
    seconds = (second_out, second_in[0], second_in[1])
    stepped = []
    for index in range(3):
        other = received[index]
        if stepped:
            other, _ = lax.optimization_barrier((other, stepped[-1][0]))
        total = split[index][0].astype(jnp.float32) + other.astype(jnp.float32)
        stepped.append(adam_update(weights[index], total, firsts[index], seconds[index]))
    out_pieces, gate_pieces, up_pieces = [gathered(step[0]) for step in stepped]
    moved_first = [move(step[1]) for step in stepped]
    moved_second = [move(step[2]) for step in stepped]

    rows = jnp.concatenate(arrived, 0)
    sides = [
        lax.dynamic_slice_in_dim(rows, dp_index * half, half, 1),
        lax.dynamic_slice_in_dim(rows, (1 - dp_index) * half, half, 1),
    ]
    totals = [jnp.zeros((rows.shape[0], half), jnp.float32) for _ in range(2)]
    for quarter in (0, 1, 2, 3):
        gate = times_rows(sides[0], gate_pieces[quarter, 0]) + times_rows(
            sides[1], gate_pieces[quarter, 1]
        )
        upward = times_rows(sides[0], up_pieces[quarter, 0]) + times_rows(
            sides[1], up_pieces[quarter, 1]
        )
        hidden = (jax.nn.silu(gate) * upward).astype(jnp.bfloat16)
        for side in range(2):
            part = jnp.dot(
                hidden, out_pieces[quarter, side], preferred_element_type=jnp.float32
            ).astype(jnp.bfloat16)
            totals[side] = totals[side] + part.astype(jnp.float32)
    own, other = [total.astype(jnp.bfloat16) for total in totals]
    results = jnp.where(
        dp_index == 0, jnp.concatenate([own, other], 1), jnp.concatenate([other, own], 1)
    ).reshape(expert_count, capacity, width)
    if relay:
        back_far = exchanged(results[3], "expert", GROUP)
        back_near = exchanged(results[1], "expert", GROUP)
        partial = weighted(far_targets, far_weight, jnp.concatenate([results[2], back_far], 0))
        arriving = exchanged(partial.astype(jnp.bfloat16), "expert", 3 * GROUP)
        combined = weighted(
            targets, combine_weight, jnp.concatenate([results[0], back_near], 0)
        ) + arriving.astype(jnp.float32)
    else:
        returned = [results[0]] + [
            exchanged(results[mask], "expert", mask * GROUP) for mask in range(1, expert_count)
        ]
        combined = weighted(targets, combine_weight, jnp.concatenate(returned, 0))
    return (
        combined.astype(jnp.bfloat16),
        jnp.stack(moved_first[1:]),
        jnp.stack(moved_second[1:]),
        moved_first[0],
        moved_second[0],
    )


def local(tokens, routes, combine_weight, owner_plan, *state):
    device_count = lax.axis_size("expert")
    expert_count = device_count // GROUP
    operands = (tokens, routes, combine_weight) + state
    if expert_count == 4:
        branches = [
            lambda *arrays, mask=mask: body(
                lambda moment: exchanged(moment, "expert", mask * GROUP), mask > 1, *arrays
            )
            for mask in range(1, expert_count)
        ]
        return lax.switch(owner_plan[0] - 1, branches, *operands)
    device_ids = jnp.arange(device_count, dtype=jnp.int32)
    source_rows = jnp.take(owner_plan, device_ids // GROUP) * GROUP + device_ids % GROUP
    return body(lambda moment: migrate_any(moment, source_rows, device_count), False, *operands)


def solution(mesh):
    in_specs = (
        P(("expert", "dp"), None),
        P(("expert", "dp"), None),
        P(("expert", "dp"), None),
        P(),
        P(None, "expert", "dp"),
        P("expert", "dp"),
        P("dp", None, "expert", None),
        P("dp", "expert", None),
        P(None, "expert", "dp"),
        P(None, "expert", "dp"),
        P("expert", "dp"),
        P("expert", "dp"),
    )
    out_specs = (
        P(("expert", "dp"), None),
        P(None, "expert", "dp"),
        P(None, "expert", "dp"),
        P("expert", "dp"),
        P("expert", "dp"),
    )
    return jax.shard_map(local, mesh=mesh, in_specs=in_specs, out_specs=out_specs, check_vma=False)
```
